32 devices in a mesh: fsdp: 4 (over y, x), head: 4 (over z), tensor: 2 (over core).
Axes of the slice: x: 2, y: 2, z: 4, core: 2. Of those that a mesh axis runs over, the one named last changes fastest.
Arguments:
- activations: bfloat16 [2, 16, 197, 768], P(None, ('fsdp', 'head')), may hold values from -6 to 6
- w_qkv: bfloat16 [3, 768, 768], P(None, 'fsdp', 'head'), may hold values from -0.21875 to 0.21875
- w_out: bfloat16 [768, 768], P('head', 'fsdp'), may hold values from -0.875 to 0.875
- gain_one: float32 [768], replicated, may hold values from 0.5 to 1.5
- gain_two: float32 [768], replicated, may hold values from 0.5 to 1.5
- w_router: bfloat16 [768, 8], replicated, may hold values from -0.15625 to 0.15625
- w_in: bfloat16 [8, 768, 3072], P('head', 'fsdp', 'tensor'), may hold values from -0.21875 to 0.21875
- w_down: bfloat16 [8, 3072, 768], P('head', 'tensor', 'fsdp'), may hold values from -0.625 to 0.625
- routes: int32 [2, 16, 197, 2], P(None, ('fsdp', 'head')), may hold values from 0 to 7, as said below
- slot_index: int32 [2, 16, 197, 2], P(None, ('fsdp', 'head')), may hold values from 0 to 63, as said below
- keep_mask: int32 [2, 16, 197, 2], P(None, ('fsdp', 'head')), may hold values from 0 to 1, as said below
- cotangent: bfloat16 [2, 16, 197, 768], P(None, ('fsdp', 'head')), may hold values from -6 to 6
Outputs:
- block_out: bfloat16 [2, 16, 197, 768], P(None, ('fsdp', 'head'))
- grad_input: float32 [2, 16, 197, 768], P(None, ('fsdp', 'head'))
- grad_qkv: float32 [3, 768, 768], P(None, 'fsdp', 'head')
- grad_out: float32 [768, 768], P('head', 'fsdp')
- grad_gain_one: float32 [768], replicated
- grad_gain_two: float32 [768], replicated
- grad_router: float32 [768, 8], replicated
- grad_in: float32 [8, 768, 3072], P('head', 'fsdp', 'tensor')
- grad_down: float32 [8, 3072, 768], P('head', 'tensor', 'fsdp')
The draws below stay inside these ranges and needn't reach their ends.
Inputs may be any that keep to these rules, and one draw needn't show every extreme that they name: `routes`: the 2 experts of a token differ. In every micro-batch and for every index of fsdp there is an expert that 72 or more rows of each device along head name. `slot_index`: among the kept pairs of one device's rows of one micro-batch that name one expert, slots are distinct. `keep_mask`: of one device's rows of one micro-batch, at most 64 pairs naming one expert are kept, and a pair is dropped only where 64 pairs of that expert are kept; in every micro-batch and index of fsdp some expert has exactly 64 kept pairs from each device along head.
All inputs are finite; a program needn't handle non-finite values.
Results may differ from the reference program's by a relative error of at most 0.02.
Values may be sent and summed in bfloat16 or wider, within the bound.
A program may use at most 192 MiB of HBM per device.

```python
import jax
import jax.numpy as jnp
from jax import lax

D = 768
HEADS = 12
HD = 64
FF = 3072
SEQ = 197
TOP = 2
EXP_DEV = 2
MICRO = 2
IMG_DEV = 1
CAP = 64
HOT = 72
EXPERTS = 8
IMAGES = 16


def route_table(key):
    blocks = MICRO * (IMAGES // IMG_DEV)
    row_count = IMG_DEV * SEQ
    members = EXPERTS // EXP_DEV
    pair_count = row_count * TOP
    keyset = jax.random.split(jax.random.fold_in(key, 7), 5)
    first_pick = jax.random.randint(keyset[0], (blocks, row_count), 0, EXPERTS)
    hot_expert = jax.random.randint(keyset[1], (blocks // members,), 0, EXPERTS)
    hot_rows = jnp.repeat(hot_expert, members)
    rank_noise = jax.random.randint(keyset[2], (blocks, row_count), 0, 1 << 20)
    ranked = jnp.argsort(jnp.argsort(rank_noise * row_count + jnp.arange(row_count)[None, :], axis=1), axis=1)
    first_pick = jnp.where(ranked < HOT, hot_rows[:, None], first_pick)
    offset = jax.random.randint(keyset[3], (blocks, row_count), 1, EXPERTS)
    second = (first_pick + offset) % EXPERTS
    routes = jnp.stack([first_pick, second], axis=-1).reshape(blocks, pair_count)
    order_noise = jax.random.randint(keyset[4], (blocks, pair_count), 0, 1 << 19)
    pair_order = jnp.argsort(order_noise * pair_count + jnp.arange(pair_count)[None, :], axis=1)
    sorted_routes = jnp.take_along_axis(routes, pair_order, axis=1)
    onehot = (sorted_routes[:, :, None] == jnp.arange(EXPERTS)[None, None, :]).astype(jnp.int32)
    position = jnp.sum((jnp.cumsum(onehot, axis=1) - 1) * onehot, axis=2)
    inverse = jnp.argsort(pair_order, axis=1)
    position = jnp.take_along_axis(position, inverse, axis=1)
    kept_pairs = (position < CAP).astype(jnp.int32)
    slot_values = position % CAP
    out_shape = (MICRO, IMAGES, SEQ, TOP)
    return (routes.reshape(out_shape).astype(jnp.int32), slot_values.reshape(out_shape).astype(jnp.int32), kept_pairs.reshape(out_shape))


def draw_routes(key, part):
    return route_table(key)[0]


def draw_slot_index(key, part):
    return route_table(key)[1]


def draw_keep_mask(key, part):
    return route_table(key)[2]


def block_levels(own_key, extent, cuts, smallest, largest):
    def one(axis_at, blocks):
        steps = jax.random.uniform(jax.random.fold_in(jax.random.fold_in(own_key, 6), axis_at), (blocks,), jnp.float32, smallest / len(cuts), largest / len(cuts))
        return jnp.repeat(jnp.exp(steps), extent[axis_at] // blocks).reshape((-1,) + (1,) * (len(extent) - axis_at - 1))

    factor_of = one(*cuts[0])
    for cut in cuts[1:]:
        factor_of = factor_of * one(*cut)
    return factor_of


def gaussian(key, shape, deviation, limit, shards=(), kind=jnp.bfloat16):
    entries = jax.random.normal(key, shape, jnp.float32) * deviation
    if len(shards) > 0:
        entries = block_levels(key, shape, shards, -0.22, 0.18) * entries
    return jnp.clip(entries, min=-limit, max=limit).astype(kind)


def setup_inputs(seed: int = 0) -> dict:
    key_of = jax.random.split(jax.random.key(seed), 13)
    activations = gaussian(key_of[0], (MICRO, IMAGES, SEQ, D), 1.0, 6.0, ((1, 16),))
    w_qkv = gaussian(key_of[1], (3, D, D), D ** -0.5, 0.21875, ((1, 4), (2, 4)))
    w_out = gaussian(key_of[2], (D, D), (D // 16) ** -0.5, 0.875, ((0, 4), (1, 4)))
    gain_one = jnp.clip(1.0 + 0.1 * jax.random.normal(key_of[3], (D,), jnp.float32), 0.5, 1.5)
    gain_two = jnp.clip(1.0 + 0.1 * jax.random.normal(key_of[4], (D,), jnp.float32), 0.5, 1.5)
    w_router = gaussian(key_of[5], (D, EXPERTS), (2 * D) ** -0.5, 0.15625)
    w_in = gaussian(key_of[6], (EXPERTS, D, FF), D ** -0.5, 0.21875, ((0, 4), (1, 4), (2, 2)))
    w_down = gaussian(key_of[7], (EXPERTS, FF, D), (FF // 32) ** -0.5, 0.625, ((0, 4), (1, 2), (2, 4)))
    routes = draw_routes(jax.random.fold_in(key_of[12], 71), 0)
    slot_index = draw_slot_index(jax.random.fold_in(key_of[12], 71), 0)
    keep_mask = draw_keep_mask(jax.random.fold_in(key_of[12], 71), 0)
    cotangent = gaussian(key_of[11], (MICRO, IMAGES, SEQ, D), 1.0, 6.0, ((1, 16),))
    return {"activations": activations, "w_qkv": w_qkv, "w_out": w_out, "gain_one": gain_one, "gain_two": gain_two, "w_router": w_router, "w_in": w_in, "w_down": w_down, "routes": routes, "slot_index": slot_index, "keep_mask": keep_mask, "cotangent": cotangent}


@jax.custom_vjp
def low(v):
    return lax.optimization_barrier(v.astype(jnp.bfloat16)).astype(jnp.float32)

@jax.custom_vjp
def low_back(v):
    return v

def low_keep(v):
    return (low(v), None)

def low_pass(kept, grad):
    return (grad,)

def back_keep(v):
    return (v, None)

def back_low(kept, grad):
    return (low(grad),)
low.defvjp(low_keep, low_pass)
low_back.defvjp(back_keep, back_low)
highest = lax.Precision.HIGHEST
norm_eps = 1e-06
group_images = 16

def norm_rows(values, gain_vec):
    centre = values - lax.optimization_barrier(jnp.mean(values, axis=-1, keepdims=True))
    spread = lax.optimization_barrier(jnp.mean(centre * centre, axis=-1, keepdims=True))
    return centre * lax.rsqrt(spread + norm_eps) * gain_vec

def attend_group(normed, w_qkv, w_out):
    image_count = normed.shape[0]
    head_shape = (image_count, SEQ, HEADS, HD)
    project = jnp.einsum('bsd,pde->pbse', normed, w_qkv, precision=highest)
    queries = low_back(low(project[0] * HD ** (-0.5))).reshape(head_shape)
    key_rows = low_back(low(project[1])).reshape(head_shape)
    value_rows = low_back(low(project[2])).reshape(head_shape)
    scores = low_back(jnp.einsum('bqhd,bkhd->bhqk', queries, key_rows, precision=highest))
    weights = low(jax.nn.softmax(scores, axis=-1))
    mixed_heads = jnp.einsum('bhqk,bkhd->bqhd', weights, value_rows, precision=highest)
    mixed_heads = low_back(low(mixed_heads.reshape(image_count, SEQ, D)))
    return jnp.einsum('bsc,cd->bsd', mixed_heads, w_out, precision=highest)

def expert_apply(block_rows, w_in_one, w_down_one):
    up_proj = low_back(jnp.dot(block_rows, w_in_one, precision=highest))
    active = low(jax.nn.gelu(up_proj, approximate=False))
    return low_back(low(jnp.dot(active, w_down_one, precision=highest)))

def forward_micro(micro_in, routes_m, slots_m, keep_m, params):
    gain_one, gain_two, w_qkv, w_out, w_router, w_in, w_down = params
    blocks = IMAGES // IMG_DEV
    row_count = IMG_DEV * SEQ
    normed = low(norm_rows(micro_in, gain_one))
    grouped = normed.reshape(IMAGES // group_images, group_images, SEQ, D)
    attend = jax.checkpoint(lambda image_block: attend_group(image_block, w_qkv, w_out))
    attended = lax.map(attend, grouped).reshape(IMAGES, SEQ, D)
    hidden = micro_in + low_back(attended)
    mixed_in = low(norm_rows(hidden, gain_two)).reshape(blocks, row_count, D)
    logits = jnp.dot(mixed_in, w_router, precision=highest)
    probs_all = jax.nn.softmax(logits, axis=-1)
    route_rows = routes_m.reshape(blocks, row_count, TOP).astype(jnp.int32)
    slot_rows = slots_m.reshape(blocks, row_count, TOP).astype(jnp.int32)
    keep_rows = keep_m.reshape(blocks, row_count, TOP).astype(jnp.float32)
    gate_values = jnp.take_along_axis(probs_all, route_rows, axis=-1) * keep_rows
    block_index = jnp.broadcast_to(jnp.arange(blocks, dtype=jnp.int32)[:, None, None], route_rows.shape)
    spread_rows = jnp.broadcast_to(mixed_in[:, :, None, :], (blocks, row_count, TOP, D)) * keep_rows[..., None]
    buffer = jnp.zeros((blocks, EXPERTS, CAP, D), jnp.float32).at[block_index, route_rows, slot_rows].add(spread_rows)
    per_expert = jnp.transpose(buffer, (1, 0, 2, 3)).reshape(EXPERTS, blocks * CAP, D)
    expert = jax.checkpoint(lambda member: expert_apply(member[0], member[1], member[2]))
    returned = lax.map(expert, (per_expert, w_in, w_down))
    returned = jnp.transpose(returned.reshape(EXPERTS, blocks, CAP, D), (1, 0, 2, 3))
    picked = returned[block_index, route_rows, slot_rows]
    moe_out = lax.optimization_barrier(jnp.sum(gate_values[..., None] * picked, axis=2))
    return hidden + moe_out.reshape(IMAGES, SEQ, D)

def reference(activations, w_qkv, w_out, gain_one, gain_two, w_router, w_in, w_down, routes, slot_index, keep_mask, cotangent):
    params = tuple((member.astype(jnp.float32) for member in (gain_one, gain_two, w_qkv, w_out, w_router, w_in, w_down)))
    inputs = activations.astype(jnp.float32)

    def forward(inputs, params):
        results = [forward_micro(inputs[micro_index], routes[micro_index], slot_index[micro_index], keep_mask[micro_index], params) for micro_index in range(MICRO)]
        return jnp.stack(results)
    result, pullback = jax.vjp(forward, inputs, params)
    grad_input, gradients = pullback(cotangent.astype(jnp.float32))
    return (result.astype(jnp.bfloat16), grad_input, gradients[2], gradients[3], gradients[0], gradients[1], gradients[4], gradients[5], gradients[6])
```

```python
import jax
import jax.numpy as jnp
from jax import lax
from jax.sharding import PartitionSpec as P

HD = 64
TOP = 2
CAP = 64

highest = lax.Precision.HIGHEST
norm_eps = 1e-06
f32 = jnp.float32
bf16 = jnp.bfloat16


def norm_rows(values, gain_vec):
    centre = values - jnp.mean(values, axis=-1, keepdims=True)
    spread = jnp.mean(centre * centre, axis=-1, keepdims=True)
    return centre * lax.rsqrt(spread + norm_eps) * gain_vec


def gelu_exact(values):
    return jax.nn.gelu(values, approximate=False)


def softmax_last(values):
    return jax.nn.softmax(values, axis=-1)


def ein(spec, left, right):
    return jnp.einsum(spec, left, right, preferred_element_type=f32)


def swap(values):
    return lax.ppermute(values, "tensor", ((0, 1), (1, 0)))


def pick(values):
    return lax.dynamic_index_in_dim(values, lax.axis_index("tensor"), 0, keepdims=False)


def both(mine):
    other = swap(mine)
    first = lax.axis_index("tensor") == 0
    return jnp.stack([jnp.where(first, mine, other), jnp.where(first, other, mine)])


def on_device(
    activations,
    w_qkv,
    w_out,
    gain_one,
    gain_two,
    w_router,
    w_in,
    w_down,
    routes,
    slot_index,
    keep_mask,
    cotangent,
):
    _, img_count, seq_length, width = activations.shape
    groups = lax.axis_size("head")
    local_heads = w_qkv.shape[2] // HD
    local_experts = w_in.shape[0]
    total_experts = local_experts * groups
    slot_count = total_experts * CAP
    tok_rows = img_count * seq_length
    head_scale = HD ** (-0.5)

    qkv_full = lax.all_gather(w_qkv, "fsdp", axis=1, tiled=True)
    out_full = lax.all_gather(w_out, "fsdp", axis=1, tiled=True)

    inputs = pick(activations).astype(f32)
    upstream = pick(cotangent).astype(f32).reshape(tok_rows, width)
    route_rows = pick(routes).reshape(tok_rows, TOP)
    slot_rows = pick(slot_index).reshape(tok_rows, TOP)
    keep_int = pick(keep_mask).reshape(tok_rows, TOP)

    normed, norm_back_one = jax.vjp(norm_rows, inputs, gain_one)
    rows_all = lax.all_gather(normed.astype(bf16), "head", axis=0, tiled=True)
    in_full = lax.all_gather(w_in, "fsdp", axis=1, tiled=True)
    down_full = lax.all_gather(w_down, "fsdp", axis=2, tiled=True)
    image_total = rows_all.shape[0]
    head_shape = (image_total, seq_length, local_heads, HD)
    project = ein("bsd,pde->pbse", rows_all, qkv_full)
    queries = (project[0] * head_scale).astype(bf16).reshape(head_shape)
    key_rows = project[1].astype(bf16).reshape(head_shape)
    value_rows = project[2].astype(bf16).reshape(head_shape)
    scores = ein("bqhd,bkhd->bhqk", queries, key_rows)
    top_score = jnp.max(scores, axis=-1, keepdims=True)
    expo_scores = jnp.exp(scores - top_score)
    row_total = jnp.sum(expo_scores, axis=-1, keepdims=True)
    attn_full = expo_scores / row_total
    attn_low = attn_full.astype(bf16)
    mixed_heads = ein("bhqk,bkhd->bqhd", attn_low, value_rows)
    mixed_heads = mixed_heads.reshape(image_total, seq_length, local_heads * HD).astype(bf16)
    partial_att = ein("bsc,cd->bsd", mixed_heads, out_full)
    attended = lax.psum_scatter(
        partial_att.astype(bf16), "head", scatter_dimension=0, tiled=True
    ).astype(f32)
    hidden = inputs + attended
    normed_two, norm_back_two = jax.vjp(norm_rows, hidden, gain_two)
    token_low = normed_two.astype(bf16).reshape(tok_rows, width)
    logits = jnp.dot(token_low, w_router, preferred_element_type=f32)
    gate_probs, softmax_back = jax.vjp(softmax_last, logits)

    keep_rows = keep_int.astype(f32)
    expert_ids = jnp.arange(total_experts, dtype=jnp.int32)
    slot_ids = jnp.arange(slot_count, dtype=jnp.int32)
    chosen = (route_rows[:, :, None] == expert_ids[None, None, :]).astype(f32)
    gate_values = jnp.sum(gate_probs[:, None, :] * chosen, axis=2) * keep_rows
    flat_slot = route_rows * CAP + slot_rows
    onehot = (
        (flat_slot.T[:, :, None] == slot_ids[None, None, :]) & (keep_int.T[:, :, None] == 1)
    ).astype(bf16)
    weighted = (gate_values.T[:, :, None] * upstream[None, :, :]).astype(bf16)
    tokens_two = jnp.broadcast_to(token_low[None], weighted.shape)
    sent = ein("ktc,ktd->cd", onehot, jnp.concatenate([tokens_two, weighted], axis=-1))
    sent = sent.astype(bf16).reshape(groups, local_experts, CAP, 2 * width)
    mine = lax.all_to_all(sent, "head", split_axis=0, concat_axis=0, tiled=True)
    slots = jnp.stack([mine, swap(mine)])
    received = slots[..., :width]
    slot_grad = slots[..., width:]

    up_proj = ein("mgecd,edf->emgcf", received, in_full)
    active, gelu_back = jax.vjp(gelu_exact, up_proj)
    active = active.astype(bf16)
    partial_out = ein("emgcf,efd->mgecd", active, down_full)
    active_grad = ein("mgecd,efd->emgcf", slot_grad, down_full)
    up_grad = gelu_back(active_grad)[0].astype(bf16)
    partial_in = ein("emgcf,edf->mgecd", up_grad, in_full)
    grad_down = ein("emgcf,mgecd->efd", active, slot_grad)
    grad_in = ein("mgecd,emgcf->edf", received, up_grad)

    partial = jnp.concatenate([partial_out, partial_in], axis=-1)
    back = (partial[0] + swap(partial[1].astype(bf16)).astype(f32)).astype(bf16)
    back = lax.all_to_all(back, "head", split_axis=0, concat_axis=0, tiled=True)
    back = back.reshape(slot_count, 2 * width)
    picked_two = ein("ktc,cd->ktd", onehot, back)
    picked = picked_two[..., :width]
    token_grad = picked_two[0, :, width:] + picked_two[1, :, width:]
    moe_out = jnp.sum(gate_values.T[:, :, None] * picked, axis=0)
    block_out = (hidden + moe_out.reshape(img_count, seq_length, width)).astype(bf16)

    gate_grad = jnp.sum(upstream[None] * picked, axis=-1).T * keep_rows
    prob_grad = jnp.sum(gate_grad[:, :, None] * chosen, axis=1)
    logit_grad = softmax_back(prob_grad)[0]
    grad_router = jnp.dot(token_low.astype(f32).T, logit_grad, precision=highest)
    token_grad = token_grad + jnp.dot(logit_grad, w_router.astype(f32).T, precision=highest)
    hidden_part, grad_gain_two = norm_back_two(token_grad.reshape(img_count, seq_length, width))
    hidden_grad = upstream.reshape(img_count, seq_length, width) + hidden_part

    att_grad_all = lax.all_gather(hidden_grad.astype(bf16), "head", axis=0, tiled=True)
    grad_out = ein("bsc,bsd->cd", mixed_heads, att_grad_all)
    mixed_grad = ein("bsd,cd->bsc", att_grad_all, out_full).astype(bf16).reshape(head_shape)
    value_grad = ein("bhqk,bqhd->bkhd", attn_low, mixed_grad).astype(bf16)
    prob_grads = ein("bqhd,bkhd->bhqk", mixed_grad, value_rows)
    row_delta = jnp.sum(prob_grads * attn_full, axis=-1, keepdims=True)
    score_grad = (attn_full * (prob_grads - row_delta)).astype(bf16)
    query_grad = (ein("bhqk,bkhd->bqhd", score_grad, key_rows) * head_scale).astype(bf16)
    key_grad = ein("bhqk,bqhd->bkhd", score_grad, queries).astype(bf16)
    proj_grad = jnp.stack([query_grad, key_grad, value_grad]).reshape(
        3, image_total, seq_length, local_heads * HD
    )
    row_part = ein("pbse,pde->bsd", proj_grad, qkv_full)
    row_grad = lax.psum_scatter(
        row_part.astype(bf16), "head", scatter_dimension=0, tiled=True
    ).astype(f32)
    grad_qkv = ein("bsd,pbse->pde", rows_all, proj_grad)
    input_part, grad_gain_one = norm_back_one(row_grad)
    input_grad = hidden_grad + input_part

    def owner(part, dim):
        part = lax.psum_scatter(part.astype(bf16), "fsdp", scatter_dimension=dim, tiled=True)
        return part

    def owner_two(part, dim):
        part = owner(part, dim)
        return part.astype(f32) + swap(part).astype(f32)

    small = lax.psum((grad_gain_one, grad_gain_two, grad_router), ("fsdp", "head", "tensor"))
    return (
        both(block_out),
        both(input_grad),
        owner_two(grad_qkv, 1),
        owner_two(grad_out, 1),
        *small,
        owner(grad_in, 1).astype(f32),
        owner(grad_down, 2).astype(f32),
    )


def solution(mesh):
    rows = P(None, ("fsdp", "head"), None, None)
    in_specs = (
        rows,
        P(None, "fsdp", "head"),
        P("head", "fsdp"),
        P(),
        P(),
        P(),
        P("head", "fsdp", "tensor"),
        P("head", "tensor", "fsdp"),
        rows,
        rows,
        rows,
        rows,
    )
    out_specs = (
        rows,
        rows,
        P(None, "fsdp", "head"),
        P("head", "fsdp"),
        P(),
        P(),
        P(),
        P("head", "fsdp", "tensor"),
        P("head", "tensor", "fsdp"),
    )
    return jax.shard_map(
        on_device, mesh=mesh, in_specs=in_specs, out_specs=out_specs, check_vma=False
    )
```
